32 devices in a mesh: curve: 8 (over z, y), seg: 4 (over x, core).
Axes of the slice: x: 2, y: 2, z: 4, core: 2. Of those that a mesh axis runs over, the one named last changes fastest.
Arguments:
- solution: bfloat16 [16384, 128], P(('curve', 'seg')), may hold values from -6 to 6
- viscosity: float32 [131072], P(('curve', 'seg')), may hold values from 0.1 to 10
- slot_index: int32 [131072, 4], P(('curve', 'seg')), may hold values from 0 to 1279, as said below
- slot_weight: int32 [131072, 4], P(('curve', 'seg')), may hold values from -1 to 8, as said below
- mirror_rows: int32 [32, 4, 192], P(('curve', 'seg')), may hold values from 0 to 511
- ghost_live: int32 [32, 4], P(('curve', 'seg')), may hold values from 0 to 192, as said below
- cell_count: int32 [32], P(('curve', 'seg')), may hold values from 512 to 4096, as said below
- viscous_block: bfloat16 [128, 128], replicated, may hold values from -0.5 to 0.5
- pressure_block: bfloat16 [128, 128], replicated, may hold values from -0.5 to 0.5
Outputs:
- residual: float32 [16384, 128], P(('curve', 'seg'))
The draws below stay inside these ranges and needn't reach their ends.
Inputs may be any that keep to these rules, and one draw needn't show every extreme that they name: `slot_index`: column 0 of each element is one of its device's owned blocks; other columns point to owned blocks or to ghost entries; ghost entries past a list's live count read zeros. `slot_weight`: each entry is one of -1, 3, 6, 8; column 0 is 8. `ghost_live`: some list is full in every draw. `cell_count`: some device is full in every draw; loads are skewed.
All inputs are finite; a program needn't handle non-finite values.
Results may differ from the reference program's by a relative error of at most 0.0035.
Values may be sent and summed in bfloat16 or wider, within the bound.
A program may use at most 64 MiB of HBM per device.

```python
import math
import jax
import jax.numpy as jnp
from jax import lax

BLOCK = 128
SLOTS = 4
REACH = 2
NB_DEV = 512
E_DEV = 4096
GHOST = 192
NOFF = 4
BLOCKS = 16384
ELEMS = 131072
N_CURVE = 8
N_SEG = 4


def draw_slot_index(key, part):
    own_key = jax.random.fold_in(key, 11)
    pick_key = jax.random.fold_in(key, 12)
    ghost_key = jax.random.fold_in(key, 13)
    owned = jax.random.randint(own_key, (ELEMS, SLOTS), 0, NB_DEV)
    ghosts = NB_DEV + jax.random.randint(ghost_key, (ELEMS, SLOTS), 0, 2 * REACH * GHOST)
    picked = jax.random.randint(pick_key, (ELEMS, SLOTS), 0, 10) < 3
    picked = picked.at[:, 0].set(False)
    return jnp.where(picked, ghosts, owned).astype(jnp.int32)


def draw_slot_weight(key, part):
    table = jnp.array([-1, 3, 6, 8], dtype=jnp.int32)
    picks = jax.random.randint(jax.random.fold_in(key, 21), (ELEMS, SLOTS), 0, 4)
    codes = table[picks]
    return codes.at[:, 0].set(8).astype(jnp.int32)


def draw_ghost_live(key, part):
    devices_all = N_CURVE * N_SEG
    counts = jax.random.randint(jax.random.fold_in(key, 31), (devices_all, 2 * REACH), 0, GHOST + 1)
    device = jax.random.randint(jax.random.fold_in(key, 32), (), 0, devices_all)
    region = jax.random.randint(jax.random.fold_in(key, 33), (), 0, 2 * REACH)
    return counts.at[device, region].set(GHOST).astype(jnp.int32)


def draw_cell_count(key, part):
    devices_all = N_CURVE * N_SEG
    full = jax.random.randint(jax.random.fold_in(key, 41), (devices_all,), 0, 8) == 0
    shifts = jax.random.randint(jax.random.fold_in(key, 42), (devices_all,), 2, 4)
    counts = jnp.where(full, E_DEV, jnp.right_shift(jnp.full((devices_all,), E_DEV, jnp.int32), shifts))
    device = jax.random.randint(jax.random.fold_in(key, 43), (), 0, devices_all)
    return counts.at[device].set(E_DEV).astype(jnp.int32)


def set_ends(drawn, key, smallest, largest):
    longest = drawn.shape.index(max(drawn.shape))
    spots = []
    for shift in (0, 1):
        where = [jax.random.randint(jax.random.fold_in(key, axis), (), 0, length) for axis, length in enumerate(drawn.shape)]
        where[longest] = (where[longest] + shift) % drawn.shape[longest]
        spots.append(tuple(where))
    return drawn.at[spots[0]].set(smallest).at[spots[1]].set(largest)


def level_of(stream_key, extent, cuts, smallest, high):
    factor_of = 1.0
    for dim, shards_of in cuts:
        heights = jax.random.uniform(jax.random.fold_in(jax.random.fold_in(stream_key, 6), dim), (shards_of,), jnp.float32, smallest / len(cuts), high / len(cuts))
        factor_of = factor_of * jnp.repeat(jnp.exp(heights), extent[dim] // shards_of).reshape((-1,) + (1,) * (len(extent) - 1 - dim))
    return factor_of


def centred(stream_key, shape, scale, most, split=(), held_as=jnp.bfloat16):
    entries = scale * jax.random.normal(stream_key, shape, jnp.float32)
    if split:
        entries = entries * level_of(stream_key, shape, split, -0.22, 0.18)
    return jnp.clip(entries, -most, most).astype(held_as)


def setup_inputs(seed: int = 0) -> dict:
    keys = jax.random.split(jax.random.key(seed), 10)
    return {
        "solution": centred(keys[0], (BLOCKS, BLOCK), 1.0, 6.0, ((0, 32),)),
        "viscosity": jnp.clip(jnp.exp(math.log(10.0) - 4.6051702 * jax.random.uniform(keys[1], (ELEMS,), jnp.float32) ** level_of(keys[1], (ELEMS,), ((0, 32),), -0.2, 0.2)), 0.1, 10.0),
        "slot_index": draw_slot_index(jax.random.fold_in(keys[9], 71), 0),
        "slot_weight": draw_slot_weight(jax.random.fold_in(keys[9], 71), 0),
        "mirror_rows": set_ends(jax.random.randint(keys[4], (N_CURVE * N_SEG, NOFF, GHOST), 0, NB_DEV), jax.random.fold_in(keys[4], 1), 0, NB_DEV - 1).astype(jnp.int32),
        "ghost_live": draw_ghost_live(jax.random.fold_in(keys[9], 71), 0),
        "cell_count": draw_cell_count(jax.random.fold_in(keys[9], 71), 0),
        "viscous_block": centred(keys[7], (BLOCK, BLOCK), BLOCK ** -0.5, 0.5),
        "pressure_block": centred(keys[8], (BLOCK, BLOCK), BLOCK ** -0.5, 0.5),
    }


def shift_list(region_count):
    return [(region // 2 + 1) * (1 if region % 2 == 0 else -1) for region in range(region_count)]


def reference(solution, viscosity, slot_index, slot_weight, mirror_rows, ghost_live, cell_count, viscous_block, pressure_block):
    devices_all = N_CURVE * N_SEG
    offsets = shift_list(2 * REACH)
    owned_all = solution.reshape(devices_all, NB_DEV, BLOCK)
    ghost_pos = jnp.arange(GHOST, dtype=jnp.int32)
    elem_pos = jnp.arange(E_DEV, dtype=jnp.int32)

    def device_part(device):
        pieces = [owned_all[device]]
        for region, offset in enumerate(offsets):
            source = device - offset
            valid = (source >= 0) & (source < devices_all)
            sender = jnp.clip(source, 0, devices_all - 1).astype(jnp.int32)
            rows = owned_all[sender][mirror_rows[sender, region]]
            keep = valid & (ghost_pos < ghost_live[sender, region])
            pieces.append(jnp.where(keep[:, None], rows, jnp.zeros_like(rows)))
        extended = jnp.concatenate(pieces, axis=0)
        start = (device * E_DEV).astype(jnp.int32)
        indices = lax.dynamic_slice_in_dim(slot_index, start, E_DEV, 0)
        codes = lax.dynamic_slice_in_dim(slot_weight, start, E_DEV, 0)
        local_visc = lax.dynamic_slice_in_dim(viscosity, start, E_DEV, 0)
        live = (elem_pos < cell_count[device]).astype(jnp.float32)
        weights = codes.astype(jnp.float32) / 8.0 * live[:, None]
        element_in = jnp.zeros((E_DEV, BLOCK), jnp.float32)
        for slot_pos in range(SLOTS):
            element_in = element_in + weights[:, slot_pos, None] * extended[indices[:, slot_pos]].astype(jnp.float32)
        element_in = element_in.astype(jnp.bfloat16)
        element_out = local_visc[:, None] * jnp.dot(element_in, viscous_block, preferred_element_type=jnp.float32)
        element_out = element_out + jnp.dot(element_in, pressure_block, preferred_element_type=jnp.float32)
        partial_value = jnp.zeros((NB_DEV + 2 * REACH * GHOST, BLOCK), jnp.float32)
        for slot_pos in range(SLOTS):
            partial_value = partial_value.at[indices[:, slot_pos]].add(weights[:, slot_pos, None] * element_out)
        return partial_value[:NB_DEV], partial_value[NB_DEV:].reshape(2 * REACH, GHOST, BLOCK)

    owned_part, ghost_part = lax.map(device_part, jnp.arange(devices_all, dtype=jnp.int32))

    def finish(device):
        total = owned_part[device]
        for region, offset in enumerate(offsets):
            target = device + offset
            valid = (target >= 0) & (target < devices_all)
            holder = jnp.clip(target, 0, devices_all - 1).astype(jnp.int32)
            piece = ghost_part[holder, region]
            keep = valid & (ghost_pos < ghost_live[device, region])
            total = total.at[mirror_rows[device, region]].add(jnp.where(keep[:, None], piece, jnp.zeros_like(piece)))
        return total

    residual = lax.map(finish, jnp.arange(devices_all, dtype=jnp.int32))
    return residual.reshape(NB_DEV * devices_all, BLOCK)
```

```python
import functools

import jax
import jax.numpy as jnp
from jax import lax
from jax.experimental import pallas as pl
from jax.experimental.pallas import tpu as pltpu
from jax.sharding import PartitionSpec as P

CHUNK = 1024
GROUP = 16
BLOCK = 64
NN = (((1,), (0,)), ((), ()))
NT = (((1,), (1,)), ((), ()))
TN = (((0,), (0,)), ((), ()))


def shift_list(region_count):
    return [(region // 2 + 1) * (1 if region % 2 == 0 else -1) for region in range(region_count)]


def mul(left, right, dims=NN):
    return lax.dot_general(left, right, dims, preferred_element_type=jnp.float32)


def kernel(
    n_curve,
    n_seg,
    ghost_rows,
    region_count,
    sol_in,
    visc_in,
    index_in,
    code_in,
    mirror_in,
    live_in,
    count_in,
    visc_mat_in,
    pres_mat_in,
    result_ref,
    sol_ref,
    visc_ref,
    index_ref,
    code_ref,
    mirror_ref,
    live_ref,
    visc_mat_ref,
    pres_mat_ref,
    count_ref,
    load_sem,
    sol_flip,
    local,
    table,
    gathered,
    elem_out,
    mirror_table,
    out_ghost,
    in_ghost,
    out_part,
    in_part,
    send_sem,
    recv_sem,
    send_back_sem,
    recv_back_sem,
):
    pairs = (
        (mirror_in, mirror_ref),
        (live_in, live_ref),
        (sol_in, sol_ref),
        (count_in, count_ref),
        (index_in, index_ref),
        (code_in, code_ref),
        (visc_mat_in, visc_mat_ref),
        (pres_mat_in, pres_mat_ref),
        (visc_in, visc_ref),
    )
    loads = [
        pltpu.make_async_copy(source, target, load_sem.at[position])
        for position, (source, target) in enumerate(pairs)
    ]
    for load in loads:
        load.start()

    devices_all = n_curve * n_seg
    owned_rows, width = sol_ref.shape
    slot_total, elem_rows = index_ref.shape
    chunk = min(CHUNK, elem_rows)
    ghost_all = ghost_rows * region_count
    offsets = shift_list(region_count)
    me = lax.axis_index("curve") * n_seg + lax.axis_index("seg")

    def exists(other):
        return jnp.logical_and(other >= 0, other < devices_all)

    def place(other):
        safe = jnp.clip(other, 0, devices_all - 1)
        return (safe // n_seg, safe % n_seg)

    barrier = pltpu.get_barrier_semaphore()
    for offset in offsets:

        @pl.when(exists(me + offset))
        def _():
            pl.semaphore_signal(
                barrier,
                inc=1,
                device_id=place(me + offset),
                device_id_type=pl.DeviceIdType.MESH,
            )

    for load in loads[:3]:
        load.wait()

    order = sorted(range(region_count), key=lambda region: -abs(offsets[region]))
    sol_flip[...] = sol_ref[...].T

    lanes = lax.broadcasted_iota(jnp.int32, (1, ghost_rows), 1)
    shape = (owned_rows // GROUP, GROUP, ghost_rows)
    position = (
        lax.broadcasted_iota(jnp.int32, shape, 0) * GROUP
        + lax.broadcasted_iota(jnp.int32, shape, 1)
    ).astype(jnp.int16)
    for region in order:
        listed = jnp.where(
            lanes < live_ref[0, region], mirror_ref[region : region + 1, :], -1
        )
        listed = jnp.broadcast_to(listed, (GROUP, ghost_rows)).astype(jnp.int16)
        hit = position == jnp.broadcast_to(listed[None], shape)
        chosen = jnp.where(hit, jnp.ones(shape, jnp.bfloat16), jnp.zeros(shape, jnp.bfloat16))
        mirror_table[region] = chosen.reshape(owned_rows, ghost_rows)
        out_ghost[pl.ds(region * ghost_rows, ghost_rows), :] = mul(
            sol_flip[...], mirror_table[region]
        ).T.astype(jnp.bfloat16)

    def ghost_copy(region, target):
        rows = pl.ds(region * ghost_rows, ghost_rows)
        return pltpu.make_async_remote_copy(
            src_ref=out_ghost.at[rows],
            dst_ref=in_ghost.at[rows],
            send_sem=send_sem.at[region],
            recv_sem=recv_sem.at[region],
            device_id=place(target),
            device_id_type=pl.DeviceIdType.MESH,
        )

    def part_copy(region, target):
        rows = pl.ds(region * ghost_rows, ghost_rows)
        return pltpu.make_async_remote_copy(
            src_ref=out_part.at[rows],
            dst_ref=in_part.at[rows],
            send_sem=send_back_sem.at[region],
            recv_sem=recv_back_sem.at[region],
            device_id=place(target),
            device_id_type=pl.DeviceIdType.MESH,
        )

    peers = sum(jnp.where(exists(me + offset), 1, 0) for offset in offsets)
    pl.semaphore_wait(barrier, peers)

    for region in order:

        @pl.when(exists(me + offsets[region]))
        def _():
            ghost_copy(region, me + offsets[region]).start()

    for region, offset in enumerate(offsets):
        rows = pl.ds(region * ghost_rows, ghost_rows)

        @pl.when(jnp.logical_not(exists(me - offset)))
        def _():
            in_ghost[rows, :] = jnp.zeros((ghost_rows, width), jnp.bfloat16)

        @pl.when(jnp.logical_not(exists(me + offset)))
        def _():
            in_part[rows, :] = jnp.zeros((ghost_rows, width), jnp.bfloat16)

    for load in loads[3:]:
        load.wait()

    applied = jnp.concatenate(
        [
            visc_mat_ref[...].astype(jnp.float32).T.astype(jnp.bfloat16),
            pres_mat_ref[...].astype(jnp.float32).T.astype(jnp.bfloat16),
        ],
        axis=1,
    )

    def table_rows(start, total, indices, weights):
        shape = (total // GROUP, GROUP, chunk)
        position = (
            lax.broadcasted_iota(jnp.int32, shape, 0) * GROUP
            + lax.broadcasted_iota(jnp.int32, shape, 1)
            + start
        ).astype(jnp.int16)
        value = jnp.zeros(shape, jnp.bfloat16)
        for index, weight in zip(indices, weights):
            hit = position == jnp.broadcast_to(index[None], shape)
            value = jnp.where(hit, jnp.broadcast_to(weight[None], shape), value)
        return value.reshape(total, chunk)

    chunks = [pl.ds(first, chunk) for first in range(0, elem_rows, chunk)]

    for step, columns in enumerate(chunks):
        element = lax.broadcasted_iota(jnp.int32, (1, chunk), 1) + step * chunk
        alive = element < count_ref[0]
        indices, weights = [], []
        for slot in range(slot_total):
            index = index_ref[slot : slot + 1, columns]
            code = code_ref[slot : slot + 1, columns].astype(jnp.float32) * 0.125
            weight = jnp.where(alive, code, 0.0)
            indices.append(jnp.broadcast_to(index, (GROUP, chunk)).astype(jnp.int16))
            weights.append(jnp.broadcast_to(weight, (GROUP, chunk)).astype(jnp.bfloat16))
        sums = []
        for slot in range(slot_total):
            value = weights[slot]
            for other in range(slot):
                same = indices[other] == indices[slot]
                value = value + jnp.where(same, weights[other], jnp.zeros_like(value))
            sums.append(value)
        for start in range(0, owned_rows, BLOCK):
            table[pl.ds(start, BLOCK), columns] = table_rows(start, BLOCK, indices, sums)
        gathered[:, columns] = mul(sol_flip[...], table[pl.ds(0, owned_rows), columns])
        for start in range(owned_rows, owned_rows + ghost_all, BLOCK):
            table[pl.ds(start, BLOCK), columns] = table_rows(
                start, BLOCK, indices[1:], sums[1:]
            )

    for turn, region in enumerate(order):
        offset = offsets[region]

        @pl.when(exists(me - offset))
        def _():
            ghost_copy(region, me - offset).wait_recv()

        rows = pl.ds(region * ghost_rows, ghost_rows)
        flipped = in_ghost[rows, :].T
        for columns in chunks:
            value = gathered[:, columns] + mul(
                flipped, table[pl.ds(owned_rows + region * ghost_rows, ghost_rows), columns]
            )
            if turn < region_count - 1:
                gathered[:, columns] = value
            else:
                element = value.astype(jnp.bfloat16)
                scaled = (element.astype(jnp.float32) * visc_ref[:, columns]).astype(jnp.bfloat16)
                pair = jnp.concatenate([scaled, element], axis=0)
                elem_out[:, columns] = mul(applied, pair).astype(jnp.bfloat16)

    for region in order:
        offset = offsets[region]
        rows = pl.ds(region * ghost_rows, ghost_rows)
        out_part[rows, :] = mul(
            elem_out[...],
            table[pl.ds(owned_rows + region * ghost_rows, ghost_rows), :],
            NT,
        ).T.astype(jnp.bfloat16)

        @pl.when(exists(me - offset))
        def _():
            part_copy(region, me - offset).start()

    local[...] = mul(elem_out[...], table[pl.ds(0, owned_rows), :], NT).T

    for region in order:
        offset = offsets[region]

        @pl.when(exists(me + offset))
        def _():
            part_copy(region, me + offset).wait_recv()

        value = local[...] + mul(
            mirror_table[region], in_part[pl.ds(region * ghost_rows, ghost_rows), :]
        )
        if region == order[-1]:
            result_ref[...] = value
        else:
            local[...] = value

    for region, offset in enumerate(offsets):

        @pl.when(exists(me + offset))
        def _():
            ghost_copy(region, me + offset).wait_send()

        @pl.when(exists(me - offset))
        def _():
            part_copy(region, me - offset).wait_send()


def per_device(
    n_curve,
    n_seg,
    solution,
    viscosity,
    slot_index,
    slot_weight,
    mirror_rows,
    ghost_live,
    cell_count,
    viscous_block,
    pressure_block,
):
    owned_rows, width = solution.shape
    region_count, ghost_rows = mirror_rows.shape[1:]
    elem_rows = viscosity.shape[0]
    ghost_all = region_count * ghost_rows
    column_total = owned_rows + ghost_all
    vmem = pl.BlockSpec(memory_space=pltpu.VMEM)
    hbm = pl.BlockSpec(memory_space=pltpu.HBM)
    ghost_buffer = pltpu.VMEM((ghost_all, width), jnp.bfloat16)
    semaphores = pltpu.SemaphoreType.DMA((region_count,))
    return pl.pallas_call(
        functools.partial(kernel, n_curve, n_seg, ghost_rows, region_count),
        out_shape=pltpu.VMEM((owned_rows, width), jnp.float32),
        in_specs=[hbm] * 9,
        out_specs=vmem,
        scratch_shapes=[
            pltpu.VMEM(solution.shape, solution.dtype),
            pltpu.VMEM((1, elem_rows), viscosity.dtype),
            pltpu.VMEM(slot_index.shape[::-1], slot_index.dtype),
            pltpu.VMEM(slot_weight.shape[::-1], slot_weight.dtype),
            pltpu.VMEM(mirror_rows.shape[1:], mirror_rows.dtype),
            pltpu.SMEM(ghost_live.shape, ghost_live.dtype),
            pltpu.VMEM(viscous_block.shape, viscous_block.dtype),
            pltpu.VMEM(pressure_block.shape, pressure_block.dtype),
            pltpu.SMEM(cell_count.shape, cell_count.dtype),
            pltpu.SemaphoreType.DMA((9,)),
            pltpu.VMEM((width, owned_rows), jnp.bfloat16),
            pltpu.VMEM((owned_rows, width), jnp.float32),
            pltpu.VMEM((column_total, elem_rows), jnp.bfloat16),
            pltpu.VMEM((width, elem_rows), jnp.float32),
            pltpu.VMEM((width, elem_rows), jnp.bfloat16),
            pltpu.VMEM((region_count, owned_rows, ghost_rows), jnp.bfloat16),
            ghost_buffer,
            ghost_buffer,
            ghost_buffer,
            ghost_buffer,
            semaphores,
            semaphores,
            semaphores,
            semaphores,
        ],
        compiler_params=pltpu.CompilerParams(
            collective_id=0, has_side_effects=True, vmem_limit_bytes=60 * 1024 * 1024
        ),
        name="stokes_operator",
    )(
        solution,
        viscosity.reshape(1, elem_rows),
        slot_index.T,
        slot_weight.T,
        mirror_rows[0],
        ghost_live,
        cell_count,
        viscous_block,
        pressure_block,
    )


def solution(mesh):
    return jax.shard_map(
        functools.partial(per_device, mesh.shape["curve"], mesh.shape["seg"]),
        mesh=mesh,
        in_specs=(
            P(("curve", "seg"), None),
            P(("curve", "seg")),
            P(("curve", "seg"), None),
            P(("curve", "seg"), None),
            P(("curve", "seg"), None, None),
            P(("curve", "seg"), None),
            P(("curve", "seg")),
            P(),
            P(),
        ),
        out_specs=P(("curve", "seg"), None),
        check_vma=False,
    )
```

```python
import functools

import jax
import jax.numpy as jnp
from jax import lax
from jax.experimental import pallas as pl
from jax.experimental.pallas import tpu as pltpu
from jax.sharding import PartitionSpec as P

CHUNK = 1024
GROUP = 16
BLOCK = 64
NN = (((1,), (0,)), ((), ()))
NT = (((1,), (1,)), ((), ()))
TN = (((0,), (0,)), ((), ()))


def shift_list(region_count):
    return [(region // 2 + 1) * (1 if region % 2 == 0 else -1) for region in range(region_count)]


def mul(left, right, dims=NN):
    return lax.dot_general(left, right, dims, preferred_element_type=jnp.float32)


def kernel(
    n_curve,
    n_seg,
    ghost_rows,
    region_count,
    sol_in,
    visc_in,
    index_in,
    code_in,
    mirror_in,
    live_in,
    count_in,
    visc_mat_in,
    pres_mat_in,
    result_ref,
    sol_ref,
    visc_ref,
    index_ref,
    code_ref,
    mirror_ref,
    live_ref,
    visc_mat_ref,
    pres_mat_ref,
    count_ref,
    load_sem,
    sol_flip,
    local,
    table,
    table_flip,
    gathered,
    elem_out,
    mirror_table,
    out_ghost,
    in_ghost,
    out_part,
    in_part,
    send_sem,
    recv_sem,
    send_back_sem,
    recv_back_sem,
):
    pairs = (
        (mirror_in, mirror_ref),
        (live_in, live_ref),
        (sol_in, sol_ref),
        (count_in, count_ref),
        (index_in, index_ref),
        (code_in, code_ref),
        (visc_mat_in, visc_mat_ref),
        (pres_mat_in, pres_mat_ref),
        (visc_in, visc_ref),
    )
    loads = [
        pltpu.make_async_copy(source, target, load_sem.at[position])
        for position, (source, target) in enumerate(pairs)
    ]
    for load in loads:
        load.start()

    devices_all = n_curve * n_seg
    owned_rows, width = sol_ref.shape
    slot_total, elem_rows = index_ref.shape
    chunk = min(CHUNK, elem_rows)
    ghost_all = ghost_rows * region_count
    offsets = shift_list(region_count)
    me = lax.axis_index("curve") * n_seg + lax.axis_index("seg")

    def exists(other):
        return jnp.logical_and(other >= 0, other < devices_all)

    def place(other):
        safe = jnp.clip(other, 0, devices_all - 1)
        return (safe // n_seg, safe % n_seg)

    barrier = pltpu.get_barrier_semaphore()
    for offset in offsets:

        @pl.when(exists(me + offset))
        def _():
            pl.semaphore_signal(
                barrier,
                inc=1,
                device_id=place(me + offset),
                device_id_type=pl.DeviceIdType.MESH,
            )

    for load in loads[:3]:
        load.wait()

    sol_flip[...] = sol_ref[...].T

    lanes = lax.broadcasted_iota(jnp.int32, (1, ghost_rows), 1)
    shape = (owned_rows // GROUP, GROUP, ghost_rows)
    position = (
        lax.broadcasted_iota(jnp.int32, shape, 0) * GROUP
        + lax.broadcasted_iota(jnp.int32, shape, 1)
    ).astype(jnp.int16)
    for region in range(region_count):
        listed = jnp.where(
            lanes < live_ref[0, region], mirror_ref[region : region + 1, :], -1
        )
        listed = jnp.broadcast_to(listed, (GROUP, ghost_rows)).astype(jnp.int16)
        hit = position == jnp.broadcast_to(listed[None], shape)
        chosen = jnp.where(hit, jnp.ones(shape, jnp.bfloat16), jnp.zeros(shape, jnp.bfloat16))
        mirror_table[region] = chosen.reshape(owned_rows, ghost_rows)
        out_ghost[pl.ds(region * ghost_rows, ghost_rows), :] = mul(
            sol_flip[...], mirror_table[region]
        ).T.astype(jnp.bfloat16)

    def offset_of(region):
        return (region // 2 + 1) * (1 - 2 * (region % 2))

    def part_rows(region):
        return pl.ds(pl.multiple_of(region * ghost_rows, GROUP), ghost_rows)

    edge = me < n_seg

    def send_order(step_of):
        near = sorted(range(region_count), key=lambda region: (abs(step_of(region)), step_of(region)))
        down = sorted(range(region_count), key=step_of)
        return near, [jnp.where(edge, first, other) for first, other in zip(down, near)]

    near_order, order = send_order(lambda region: offsets[region])
    back_near, back_order = send_order(lambda region: -offsets[region])

    def ghost_copy(region, target):
        rows = part_rows(region)
        return pltpu.make_async_remote_copy(
            src_ref=out_ghost.at[rows],
            dst_ref=in_ghost.at[rows],
            send_sem=send_sem.at[region],
            recv_sem=recv_sem.at[region],
            device_id=place(target),
            device_id_type=pl.DeviceIdType.MESH,
        )

    def part_copy(region, target):
        rows = part_rows(region)
        return pltpu.make_async_remote_copy(
            src_ref=out_part.at[rows],
            dst_ref=in_part.at[rows],
            send_sem=send_back_sem.at[region],
            recv_sem=recv_back_sem.at[region],
            device_id=place(target),
            device_id_type=pl.DeviceIdType.MESH,
        )

    peers = sum(jnp.where(exists(me + offset), 1, 0) for offset in offsets)
    pl.semaphore_wait(barrier, peers)

    for region in order:

        @pl.when(exists(me + offset_of(region)))
        def _():
            ghost_copy(region, me + offset_of(region)).start()

    for region, offset in enumerate(offsets):
        rows = pl.ds(region * ghost_rows, ghost_rows)

        @pl.when(jnp.logical_not(exists(me - offset)))
        def _():
            in_ghost[rows, :] = jnp.zeros((ghost_rows, width), jnp.bfloat16)

        @pl.when(jnp.logical_not(exists(me + offset)))
        def _():
            in_part[rows, :] = jnp.zeros((ghost_rows, width), jnp.bfloat16)

    for load in loads[3:]:
        load.wait()

    applied = jnp.concatenate(
        [
            visc_mat_ref[...].astype(jnp.float32).T.astype(jnp.bfloat16),
            pres_mat_ref[...].astype(jnp.float32).T.astype(jnp.bfloat16),
        ],
        axis=1,
    )

    def table_rows(start, total, indices, weights):
        shape = (total // GROUP, GROUP, chunk)
        position = (
            lax.broadcasted_iota(jnp.int32, shape, 0) * GROUP
            + lax.broadcasted_iota(jnp.int32, shape, 1)
            + start
        ).astype(jnp.int16)
        value = jnp.zeros(shape, jnp.bfloat16)
        for index, weight in zip(indices, weights):
            hit = position == jnp.broadcast_to(index[None], shape)
            value = jnp.where(hit, jnp.broadcast_to(weight[None], shape), value)
        return value.reshape(total, chunk)

    chunks = [pl.ds(first, chunk) for first in range(0, elem_rows, chunk)]

    for step, columns in enumerate(chunks):
        element = lax.broadcasted_iota(jnp.int32, (1, chunk), 1) + step * chunk
        alive = element < count_ref[0]
        indices, weights = [], []
        for slot in range(slot_total):
            index = index_ref[slot : slot + 1, columns]
            code = code_ref[slot : slot + 1, columns].astype(jnp.float32) * 0.125
            weight = jnp.where(alive, code, 0.0)
            indices.append(jnp.broadcast_to(index, (GROUP, chunk)).astype(jnp.int16))
            weights.append(jnp.broadcast_to(weight, (GROUP, chunk)).astype(jnp.bfloat16))
        sums = []
        for slot in range(slot_total):
            value = weights[slot]
            for other in range(slot):
                same = indices[other] == indices[slot]
                value = value + jnp.where(same, weights[other], jnp.zeros_like(value))
            sums.append(value)
        for start in range(0, owned_rows, BLOCK):
            table[pl.ds(start, BLOCK), columns] = table_rows(start, BLOCK, indices, sums)
        gathered[:, columns] = mul(sol_flip[...], table[pl.ds(0, owned_rows), columns])
        for start in range(owned_rows, owned_rows + ghost_all, BLOCK):
            table[pl.ds(start, BLOCK), columns] = table_rows(
                start, BLOCK, indices[1:], sums[1:]
            )
        for region in range(region_count):
            first = owned_rows + region * ghost_rows
            table_flip[region, columns, :] = table[pl.ds(first, ghost_rows), columns].T

    values = [gathered[:, columns] for columns in chunks]
    for region in near_order:

        @pl.when(exists(me - offset_of(region)))
        def _():
            ghost_copy(region, me - offset_of(region)).wait_recv()

        flipped = in_ghost[part_rows(region), :].T
        first = owned_rows + region * ghost_rows
        values = [
            value + mul(flipped, table[pl.ds(first, ghost_rows), columns])
            for value, columns in zip(values, chunks)
        ]
    pairs = []
    for value, columns in zip(values, chunks):
        element = value.astype(jnp.bfloat16)
        scaled = (element.astype(jnp.float32) * visc_ref[:, columns]).astype(jnp.bfloat16)
        pairs.append(jnp.concatenate([scaled, element], axis=0))
    for pair, columns in zip(pairs, chunks):
        elem_out[:, columns] = mul(applied, pair).astype(jnp.bfloat16)

    for group in (back_order[:2], back_order[2:]):
        parts = [mul(elem_out[...], table_flip[region]) for region in group]
        for region, part in zip(group, parts):
            out_part[part_rows(region), :] = part.T.astype(jnp.bfloat16)
        for region in group:

            @pl.when(exists(me - offset_of(region)))
            def _():
                part_copy(region, me - offset_of(region)).start()

    local[...] = mul(elem_out[...], table[pl.ds(0, owned_rows), :], NT).T

    total = local[...]
    for group in (back_near[:2], back_near[2:]):
        for region in group:

            @pl.when(exists(me + offsets[region]))
            def _():
                part_copy(region, me + offsets[region]).wait_recv()

        total = total + sum(
            mul(mirror_table[region], in_part[part_rows(region), :]) for region in group
        )
    result_ref[...] = total

    for region, offset in enumerate(offsets):

        @pl.when(exists(me + offset))
        def _():
            ghost_copy(region, me + offset).wait_send()

        @pl.when(exists(me - offset))
        def _():
            part_copy(region, me - offset).wait_send()


def per_device(
    n_curve,
    n_seg,
    solution,
    viscosity,
    slot_index,
    slot_weight,
    mirror_rows,
    ghost_live,
    cell_count,
    viscous_block,
    pressure_block,
):
    owned_rows, width = solution.shape
    region_count, ghost_rows = mirror_rows.shape[1:]
    elem_rows = viscosity.shape[0]
    ghost_all = region_count * ghost_rows
    column_total = owned_rows + ghost_all
    vmem = pl.BlockSpec(memory_space=pltpu.VMEM)
    hbm = pl.BlockSpec(memory_space=pltpu.HBM)
    ghost_buffer = pltpu.VMEM((ghost_all, width), jnp.bfloat16)
    semaphores = pltpu.SemaphoreType.DMA((region_count,))
    return pl.pallas_call(
        functools.partial(kernel, n_curve, n_seg, ghost_rows, region_count),
        out_shape=pltpu.VMEM((owned_rows, width), jnp.float32),
        in_specs=[hbm] * 9,
        out_specs=vmem,
        scratch_shapes=[
            pltpu.VMEM(solution.shape, solution.dtype),
            pltpu.VMEM((1, elem_rows), viscosity.dtype),
            pltpu.VMEM(slot_index.shape[::-1], slot_index.dtype),
            pltpu.VMEM(slot_weight.shape[::-1], slot_weight.dtype),
            pltpu.VMEM(mirror_rows.shape[1:], mirror_rows.dtype),
            pltpu.SMEM(ghost_live.shape, ghost_live.dtype),
            pltpu.VMEM(viscous_block.shape, viscous_block.dtype),
            pltpu.VMEM(pressure_block.shape, pressure_block.dtype),
            pltpu.SMEM(cell_count.shape, cell_count.dtype),
            pltpu.SemaphoreType.DMA((9,)),
            pltpu.VMEM((width, owned_rows), jnp.bfloat16),
            pltpu.VMEM((owned_rows, width), jnp.float32),
            pltpu.VMEM((column_total, elem_rows), jnp.bfloat16),
            pltpu.VMEM((region_count, elem_rows, ghost_rows), jnp.bfloat16),
            pltpu.VMEM((width, elem_rows), jnp.float32),
            pltpu.VMEM((width, elem_rows), jnp.bfloat16),
            pltpu.VMEM((region_count, owned_rows, ghost_rows), jnp.bfloat16),
            ghost_buffer,
            ghost_buffer,
            ghost_buffer,
            ghost_buffer,
            semaphores,
            semaphores,
            semaphores,
            semaphores,
        ],
        compiler_params=pltpu.CompilerParams(
            collective_id=0, has_side_effects=True, vmem_limit_bytes=60 * 1024 * 1024
        ),
        name="stokes_operator",
    )(
        solution,
        viscosity.reshape(1, elem_rows),
        slot_index.T,
        slot_weight.T,
        mirror_rows[0],
        ghost_live,
        cell_count,
        viscous_block,
        pressure_block,
    )


def solution(mesh):
    return jax.shard_map(
        functools.partial(per_device, mesh.shape["curve"], mesh.shape["seg"]),
        mesh=mesh,
        in_specs=(
            P(("curve", "seg"), None),
            P(("curve", "seg")),
            P(("curve", "seg"), None),
            P(("curve", "seg"), None),
            P(("curve", "seg"), None, None),
            P(("curve", "seg"), None),
            P(("curve", "seg")),
            P(),
            P(),
        ),
        out_specs=P(("curve", "seg"), None),
        check_vma=False,
    )
```

```python
import functools

import jax
import jax.numpy as jnp
from jax import lax
from jax.experimental import pallas as pl
from jax.experimental.pallas import tpu as pltpu
from jax.sharding import PartitionSpec as P

CHUNK = 1024
GROUP = 16
BLOCK = 64
NN = (((1,), (0,)), ((), ()))
NT = (((1,), (1,)), ((), ()))
TN = (((0,), (0,)), ((), ()))


def shift_list(region_count):
    return [(region // 2 + 1) * (1 if region % 2 == 0 else -1) for region in range(region_count)]


def mul(left, right, dims=NN):
    return lax.dot_general(left, right, dims, preferred_element_type=jnp.float32)


def kernel(
    n_curve,
    n_seg,
    ghost_rows,
    region_count,
    sol_in,
    visc_in,
    index_in,
    code_in,
    mirror_in,
    live_in,
    count_in,
    visc_mat_in,
    pres_mat_in,
    result_ref,
    sol_ref,
    visc_ref,
    index_ref,
    code_ref,
    mirror_ref,
    live_ref,
    visc_mat_ref,
    pres_mat_ref,
    count_ref,
    load_sem,
    sol_flip,
    local,
    table,
    table_flip,
    gathered,
    elem_out,
    mirror_table,
    out_ghost,
    in_ghost,
    out_part,
    in_part,
    send_sem,
    recv_sem,
    send_back_sem,
    recv_back_sem,
):
    pairs = (
        (mirror_in, mirror_ref),
        (live_in, live_ref),
        (sol_in, sol_ref),
        (count_in, count_ref),
        (index_in, index_ref),
        (code_in, code_ref),
        (visc_mat_in, visc_mat_ref),
        (pres_mat_in, pres_mat_ref),
        (visc_in, visc_ref),
    )
    devices_all = n_curve * n_seg
    owned_rows, width = sol_ref.shape
    slot_total, elem_rows = index_ref.shape
    chunk = min(CHUNK, elem_rows)
    ghost_all = ghost_rows * region_count
    offsets = shift_list(region_count)
    me = lax.axis_index("curve") * n_seg + lax.axis_index("seg")

    def exists(other):
        return jnp.logical_and(other >= 0, other < devices_all)

    def place(other):
        safe = jnp.clip(other, 0, devices_all - 1)
        return (safe // n_seg, safe % n_seg)

    barrier = pltpu.get_barrier_semaphore()
    for offset in offsets[::-1]:

        @pl.when(exists(me + offset))
        def _():
            pl.semaphore_signal(
                barrier,
                inc=1,
                device_id=place(me + offset),
                device_id_type=pl.DeviceIdType.MESH,
            )

    loads = [
        pltpu.make_async_copy(source, target, load_sem.at[position])
        for position, (source, target) in enumerate(pairs)
    ]
    for load in loads:
        load.start()

    for load in loads[:3]:
        load.wait()

    sol_flip[...] = sol_ref[...].T

    lanes = lax.broadcasted_iota(jnp.int32, (1, ghost_rows), 1)
    shape = (owned_rows // GROUP, GROUP, ghost_rows)
    position = (
        lax.broadcasted_iota(jnp.int32, shape, 0) * GROUP
        + lax.broadcasted_iota(jnp.int32, shape, 1)
    ).astype(jnp.int16)
    for region in range(region_count):
        listed = jnp.where(
            lanes < live_ref[0, region], mirror_ref[region : region + 1, :], -1
        )
        listed = jnp.broadcast_to(listed, (GROUP, ghost_rows)).astype(jnp.int16)
        hit = position == jnp.broadcast_to(listed[None], shape)
        chosen = jnp.where(hit, jnp.ones(shape, jnp.bfloat16), jnp.zeros(shape, jnp.bfloat16))
        mirror_table[region] = chosen.reshape(owned_rows, ghost_rows)
        out_ghost[pl.ds(region * ghost_rows, ghost_rows), :] = mul(
            sol_flip[...], mirror_table[region]
        ).T.astype(jnp.bfloat16)

    def offset_of(region):
        return (region // 2 + 1) * (1 - 2 * (region % 2))

    def part_rows(region):
        return pl.ds(pl.multiple_of(region * ghost_rows, GROUP), ghost_rows)

    regions = list(range(region_count))
    edge = me < n_seg
    odd = me % 2 == 1
    near_order = sorted(regions, key=lambda region: (abs(offsets[region]), offsets[region]))
    down_order = sorted(regions, key=lambda region: offsets[region])
    order = [jnp.where(edge, *pair) for pair in zip(down_order, near_order)]

    def back_key(partner, by_step):
        def key(region):
            step = -offsets[region]
            return (step == partner, step if by_step else abs(step), step)

        return key

    even_rest, odd_rest, even_edge, odd_edge = (
        sorted(regions, key=back_key(partner, by_step))
        for by_step in (False, True)
        for partner in (1, -1)
    )
    back_order = [
        jnp.where(edge, jnp.where(odd, first, second), jnp.where(odd, third, fourth))
        for first, second, third, fourth in zip(odd_edge, even_edge, odd_rest, even_rest)
    ]

    def ghost_copy(region, target):
        rows = part_rows(region)
        return pltpu.make_async_remote_copy(
            src_ref=out_ghost.at[rows],
            dst_ref=in_ghost.at[rows],
            send_sem=send_sem.at[region],
            recv_sem=recv_sem.at[region],
            device_id=place(target),
            device_id_type=pl.DeviceIdType.MESH,
        )

    def part_copy(region, target):
        rows = part_rows(region)
        return pltpu.make_async_remote_copy(
            src_ref=out_part.at[rows],
            dst_ref=in_part.at[rows],
            send_sem=send_back_sem.at[region],
            recv_sem=recv_back_sem.at[region],
            device_id=place(target),
            device_id_type=pl.DeviceIdType.MESH,
        )

    peers = sum(jnp.where(exists(me + offset), 1, 0) for offset in offsets)
    pl.semaphore_wait(barrier, peers)

    for region in order:

        @pl.when(exists(me + offset_of(region)))
        def _():
            ghost_copy(region, me + offset_of(region)).start()

    for region, offset in enumerate(offsets):
        rows = pl.ds(region * ghost_rows, ghost_rows)

        @pl.when(jnp.logical_not(exists(me - offset)))
        def _():
            in_ghost[rows, :] = jnp.zeros((ghost_rows, width), jnp.bfloat16)

        @pl.when(jnp.logical_not(exists(me + offset)))
        def _():
            in_part[rows, :] = jnp.zeros((ghost_rows, width), jnp.bfloat16)

    for load in loads[3:]:
        load.wait()

    applied = jnp.concatenate(
        [
            visc_mat_ref[...].astype(jnp.float32).T.astype(jnp.bfloat16),
            pres_mat_ref[...].astype(jnp.float32).T.astype(jnp.bfloat16),
        ],
        axis=1,
    )

    def table_rows(start, total, indices, weights):
        shape = (total // GROUP, GROUP, chunk)
        position = (
            lax.broadcasted_iota(jnp.int32, shape, 0) * GROUP
            + lax.broadcasted_iota(jnp.int32, shape, 1)
            + start
        ).astype(jnp.int16)
        value = jnp.zeros(shape, jnp.bfloat16)
        for index, weight in zip(indices, weights):
            hit = position == jnp.broadcast_to(index[None], shape)
            value = jnp.where(hit, jnp.broadcast_to(weight[None], shape), value)
        return value.reshape(total, chunk)

    chunks = [pl.ds(first, chunk) for first in range(0, elem_rows, chunk)]

    for step, columns in enumerate(chunks):
        element = lax.broadcasted_iota(jnp.int32, (1, chunk), 1) + step * chunk
        alive = element < count_ref[0]
        indices, weights = [], []
        for slot in range(slot_total):
            index = index_ref[slot : slot + 1, columns]
            code = code_ref[slot : slot + 1, columns].astype(jnp.float32) * 0.125
            weight = jnp.where(alive, code, 0.0)
            indices.append(jnp.broadcast_to(index, (GROUP, chunk)).astype(jnp.int16))
            weights.append(jnp.broadcast_to(weight, (GROUP, chunk)).astype(jnp.bfloat16))
        sums = []
        for slot in range(slot_total):
            value = weights[slot]
            for other in range(slot):
                same = indices[other] == indices[slot]
                value = value + jnp.where(same, weights[other], jnp.zeros_like(value))
            sums.append(value)
        for start in range(0, owned_rows, BLOCK):
            table[pl.ds(start, BLOCK), columns] = table_rows(start, BLOCK, indices, sums)
        gathered[:, columns] = mul(sol_flip[...], table[pl.ds(0, owned_rows), columns])
        for start in range(owned_rows, owned_rows + ghost_all, BLOCK):
            table[pl.ds(start, BLOCK), columns] = table_rows(
                start, BLOCK, indices[1:], sums[1:]
            )
        for region in range(region_count):
            first = owned_rows + region * ghost_rows
            table_flip[region, columns, :] = table[pl.ds(first, ghost_rows), columns].T

    values = [gathered[:, columns] for columns in chunks]
    for group in (near_order,):
        for region in group:

            @pl.when(exists(me - offset_of(region)))
            def _():
                ghost_copy(region, me - offset_of(region)).wait_recv()

        first, count = min(group) * ghost_rows, len(group) * ghost_rows
        flipped = in_ghost[pl.ds(first, count), :].T
        values = [
            value + mul(flipped, table[pl.ds(owned_rows + first, count), columns])
            for value, columns in zip(values, chunks)
        ]
    pairs = []
    for value, columns in zip(values, chunks):
        element = value.astype(jnp.bfloat16)
        scaled = (element.astype(jnp.float32) * visc_ref[:, columns]).astype(jnp.bfloat16)
        pairs.append(jnp.concatenate([scaled, element], axis=0))
    for pair, columns in zip(pairs, chunks):
        elem_out[:, columns] = mul(applied, pair).astype(jnp.bfloat16)

    half = elem_rows // 2

    def scatter(region):
        return [
            mul(elem_out[:, rows], table_flip[region, rows, :])
            for rows in (pl.ds(0, half), pl.ds(half, half))
        ]

    coming = scatter(back_order[0])
    for turn, region in enumerate(back_order):
        front, back = coming
        if turn < region_count - 1:
            coming = scatter(back_order[turn + 1])
        out_part[part_rows(region), :] = (front.T + back.T).astype(jnp.bfloat16)

        @pl.when(exists(me - offset_of(region)))
        def _():
            part_copy(region, me - offset_of(region)).start()

    local[...] = mul(elem_out[...], table[pl.ds(0, owned_rows), :], NT).T

    halves = [pl.ds(first, owned_rows // 2) for first in (0, owned_rows // 2)]
    totals = [local[rows, :] for rows in halves]
    for group in (regions[:2], regions[2:]):
        for region in group:

            @pl.when(exists(me + offsets[region]))
            def _():
                part_copy(region, me + offsets[region]).wait_recv()

        totals = [
            total
            + sum(mul(mirror_table[region, rows, :], in_part[part_rows(region), :]) for region in group)
            for total, rows in zip(totals, halves)
        ]
    for total, rows in zip(totals, halves):
        result_ref[rows, :] = total

    for region, offset in enumerate(offsets):

        @pl.when(exists(me + offset))
        def _():
            ghost_copy(region, me + offset).wait_send()

        @pl.when(exists(me - offset))
        def _():
            part_copy(region, me - offset).wait_send()


def per_device(
    n_curve,
    n_seg,
    solution,
    viscosity,
    slot_index,
    slot_weight,
    mirror_rows,
    ghost_live,
    cell_count,
    viscous_block,
    pressure_block,
):
    owned_rows, width = solution.shape
    region_count, ghost_rows = mirror_rows.shape[1:]
    elem_rows = viscosity.shape[0]
    ghost_all = region_count * ghost_rows
    column_total = owned_rows + ghost_all
    vmem = pl.BlockSpec(memory_space=pltpu.VMEM)
    hbm = pl.BlockSpec(memory_space=pltpu.HBM)
    ghost_buffer = pltpu.VMEM((ghost_all, width), jnp.bfloat16)
    semaphores = pltpu.SemaphoreType.DMA((region_count,))
    return pl.pallas_call(
        functools.partial(kernel, n_curve, n_seg, ghost_rows, region_count),
        out_shape=pltpu.VMEM((owned_rows, width), jnp.float32),
        in_specs=[hbm] * 9,
        out_specs=vmem,
        scratch_shapes=[
            pltpu.VMEM(solution.shape, solution.dtype),
            pltpu.VMEM((1, elem_rows), viscosity.dtype),
            pltpu.VMEM(slot_index.shape[::-1], slot_index.dtype),
            pltpu.VMEM(slot_weight.shape[::-1], slot_weight.dtype),
            pltpu.VMEM(mirror_rows.shape[1:], mirror_rows.dtype),
            pltpu.SMEM(ghost_live.shape, ghost_live.dtype),
            pltpu.VMEM(viscous_block.shape, viscous_block.dtype),
            pltpu.VMEM(pressure_block.shape, pressure_block.dtype),
            pltpu.SMEM(cell_count.shape, cell_count.dtype),
            pltpu.SemaphoreType.DMA((9,)),
            pltpu.VMEM((width, owned_rows), jnp.bfloat16),
            pltpu.VMEM((owned_rows, width), jnp.float32),
            pltpu.VMEM((column_total, elem_rows), jnp.bfloat16),
            pltpu.VMEM((region_count, elem_rows, ghost_rows), jnp.bfloat16),
            pltpu.VMEM((width, elem_rows), jnp.float32),
            pltpu.VMEM((width, elem_rows), jnp.bfloat16),
            pltpu.VMEM((region_count, owned_rows, ghost_rows), jnp.bfloat16),
            ghost_buffer,
            ghost_buffer,
            ghost_buffer,
            ghost_buffer,
            semaphores,
            semaphores,
            semaphores,
            semaphores,
        ],
        compiler_params=pltpu.CompilerParams(
            collective_id=0, has_side_effects=True, vmem_limit_bytes=60 * 1024 * 1024
        ),
        name="stokes_operator",
    )(
        solution,
        viscosity.reshape(1, elem_rows),
        slot_index.T,
        slot_weight.T,
        mirror_rows[0],
        ghost_live,
        cell_count,
        viscous_block,
        pressure_block,
    )


def solution(mesh):
    return jax.shard_map(
        functools.partial(per_device, mesh.shape["curve"], mesh.shape["seg"]),
        mesh=mesh,
        in_specs=(
            P(("curve", "seg"), None),
            P(("curve", "seg")),
            P(("curve", "seg"), None),
            P(("curve", "seg"), None),
            P(("curve", "seg"), None, None),
            P(("curve", "seg"), None),
            P(("curve", "seg")),
            P(),
            P(),
        ),
        out_specs=P(("curve", "seg"), None),
        check_vma=False,
    )
```

```python
import functools

import jax
import jax.numpy as jnp
from jax import lax
from jax.experimental import pallas as pl
from jax.experimental.pallas import tpu as pltpu
from jax.sharding import PartitionSpec as P

CHUNK = 1024
GROUP = 16
BLOCK = 64
TILE = 256
HEAD = 128
NN = (((1,), (0,)), ((), ()))
NT = (((1,), (1,)), ((), ()))
TN = (((0,), (0,)), ((), ()))


def shift_list(region_count):
    return [(region // 2 + 1) * (1 if region % 2 == 0 else -1) for region in range(region_count)]


def mul(left, right, dims=NN):
    return lax.dot_general(left, right, dims, preferred_element_type=jnp.float32)


def kernel(
    n_curve,
    n_seg,
    ghost_rows,
    region_count,
    sol_in,
    visc_in,
    index_in,
    code_in,
    mirror_in,
    live_in,
    count_in,
    visc_mat_in,
    pres_mat_in,
    result_ref,
    sol_ref,
    visc_ref,
    index_ref,
    code_ref,
    mirror_ref,
    live_ref,
    visc_mat_ref,
    pres_mat_ref,
    count_ref,
    load_sem,
    sol_flip,
    local,
    table,
    table_flip,
    gathered,
    elem_out,
    mirror_table,
    out_ghost,
    in_ghost,
    out_part,
    in_part,
    send_sem,
    recv_sem,
    send_back_sem,
    recv_back_sem,
):
    pairs = (
        (mirror_in, mirror_ref),
        (live_in, live_ref),
        (sol_in, sol_ref),
        (count_in, count_ref),
        (index_in, index_ref),
        (code_in, code_ref),
        (visc_mat_in, visc_mat_ref),
        (pres_mat_in, pres_mat_ref),
        (visc_in, visc_ref),
    )
    devices_all = n_curve * n_seg
    owned_rows, width = sol_ref.shape
    slot_total, elem_rows = index_ref.shape
    chunk = min(CHUNK, elem_rows)
    ghost_all = ghost_rows * region_count
    offsets = shift_list(region_count)
    me = lax.axis_index("curve") * n_seg + lax.axis_index("seg")

    def exists(other):
        return jnp.logical_and(other >= 0, other < devices_all)

    def place(other):
        safe = jnp.clip(other, 0, devices_all - 1)
        return (safe // n_seg, safe % n_seg)

    barrier = pltpu.get_barrier_semaphore()
    for offset in offsets[::-1]:

        @pl.when(exists(me + offset))
        def _():
            pl.semaphore_signal(
                barrier,
                inc=1,
                device_id=place(me + offset),
                device_id_type=pl.DeviceIdType.MESH,
            )

    loads = [
        pltpu.make_async_copy(source, target, load_sem.at[position])
        for position, (source, target) in enumerate(pairs)
    ]
    for load in loads:
        load.start()

    for load in loads[:6]:
        load.wait()

    def table_rows(start, total, indices, weights):
        shape = (total // GROUP, GROUP, chunk)
        position = (
            lax.broadcasted_iota(jnp.int32, shape, 0) * GROUP
            + lax.broadcasted_iota(jnp.int32, shape, 1)
            + start
        ).astype(jnp.int16)
        value = jnp.zeros(shape, jnp.bfloat16)
        for index, weight in zip(indices, weights):
            hit = position == jnp.broadcast_to(index[None], shape)
            value = jnp.where(hit, jnp.broadcast_to(weight[None], shape), value)
        return value.reshape(total, chunk)

    chunks = [pl.ds(first, chunk) for first in range(0, elem_rows, chunk)]

    def prepare(step, columns):
        element = lax.broadcasted_iota(jnp.int32, (1, chunk), 1) + step * chunk
        alive = element < count_ref[0]
        indices, weights = [], []
        for slot in range(slot_total):
            index = index_ref[slot : slot + 1, columns]
            code = code_ref[slot : slot + 1, columns].astype(jnp.float32) * 0.125
            weight = jnp.where(alive, code, 0.0)
            indices.append(jnp.broadcast_to(index, (GROUP, chunk)).astype(jnp.int16))
            weights.append(jnp.broadcast_to(weight, (GROUP, chunk)).astype(jnp.bfloat16))
        sums = []
        for slot in range(slot_total):
            value = weights[slot]
            for other in range(slot):
                same = indices[other] == indices[slot]
                value = value + jnp.where(same, weights[other], jnp.zeros_like(value))
            sums.append(value)
        return indices, sums

    def fill_owned(columns, first, last, ready):
        for start in range(first, last, BLOCK):
            table[pl.ds(start, BLOCK), columns] = table_rows(start, BLOCK, *ready)

    sol_flip[...] = sol_ref[...].T

    lanes = lax.broadcasted_iota(jnp.int32, (1, ghost_rows), 1)
    shape = (owned_rows // GROUP, GROUP, ghost_rows)
    position = (
        lax.broadcasted_iota(jnp.int32, shape, 0) * GROUP
        + lax.broadcasted_iota(jnp.int32, shape, 1)
    ).astype(jnp.int16)
    for region in range(region_count):
        listed = jnp.where(
            lanes < live_ref[0, region], mirror_ref[region : region + 1, :], -1
        )
        listed = jnp.broadcast_to(listed, (GROUP, ghost_rows)).astype(jnp.int16)
        hit = position == jnp.broadcast_to(listed[None], shape)
        chosen = jnp.where(hit, jnp.ones(shape, jnp.bfloat16), jnp.zeros(shape, jnp.bfloat16))
        mirror_table[region] = chosen.reshape(owned_rows, ghost_rows)
        out_ghost[pl.ds(region * ghost_rows, ghost_rows), :] = mul(
            sol_flip[...], mirror_table[region]
        ).T.astype(jnp.bfloat16)

    prepared = prepare(0, chunks[0])
    fill_owned(chunks[0], 0, HEAD, prepared)

    def offset_of(region):
        return (region // 2 + 1) * (1 - 2 * (region % 2))

    def part_rows(region):
        return pl.ds(pl.multiple_of(region * ghost_rows, GROUP), ghost_rows)

    regions = list(range(region_count))
    edge = me < n_seg
    odd = me % 2
    incoming = [1 - odd, odd] + regions[2:]
    outgoing = [odd, 1 - odd] + regions[2:]
    lead = -ghost_rows % TILE
    early = ghost_rows + lead
    pieces = [(0, 0, ghost_rows), (1, 0, lead), (1, lead, ghost_rows - lead)]
    pieces += [(slot, 0, ghost_rows) for slot in regions[2:]]

    def piece_copy(number):
        slot, first, count = pieces[number]
        source = pl.multiple_of(outgoing[slot] * ghost_rows + first, GROUP)
        return pltpu.make_async_remote_copy(
            src_ref=out_ghost.at[pl.ds(source, count)],
            dst_ref=in_ghost.at[pl.ds(slot * ghost_rows + first, count)],
            send_sem=send_sem.at[number],
            recv_sem=recv_sem.at[number],
            device_id=place(me + offset_of(outgoing[slot])),
            device_id_type=pl.DeviceIdType.MESH,
        )

    def has_target(number):
        return exists(me + offset_of(outgoing[pieces[number][0]]))

    def has_source(number):
        return exists(me - offset_of(incoming[pieces[number][0]]))

    def incoming_of(slot):
        return jnp.where(slot < 2, (1 - slot) * (1 - odd) + slot * odd, slot)

    def part_copy(slot):
        region = incoming_of(slot)
        return pltpu.make_async_remote_copy(
            src_ref=out_part.at[part_rows(slot)],
            dst_ref=in_part.at[part_rows(region)],
            send_sem=send_back_sem.at[slot],
            recv_sem=recv_back_sem.at[region],
            device_id=place(me - offset_of(region)),
            device_id_type=pl.DeviceIdType.MESH,
        )

    def part_arrival(region):
        return pltpu.make_async_remote_copy(
            src_ref=out_part.at[part_rows(region)],
            dst_ref=in_part.at[part_rows(region)],
            send_sem=send_back_sem.at[region],
            recv_sem=recv_back_sem.at[region],
            device_id=place(me + offsets[region]),
            device_id_type=pl.DeviceIdType.MESH,
        )

    peers = sum(jnp.where(exists(me + offset), 1, 0) for offset in offsets)
    pl.semaphore_wait(barrier, peers)

    for number in (1, 0, 2, *range(len(pieces) - 1, 2, -1)):

        @pl.when(has_target(number))
        def _():
            piece_copy(number).start()

    for number, (slot, first, count) in enumerate(pieces):

        @pl.when(jnp.logical_not(has_source(number)))
        def _():
            in_ghost[pl.ds(slot * ghost_rows + first, count), :] = jnp.zeros(
                (count, width), jnp.bfloat16
            )

    for region, offset in enumerate(offsets):

        @pl.when(jnp.logical_not(exists(me + offset)))
        def _():
            in_part[part_rows(region), :] = jnp.zeros((ghost_rows, width), jnp.bfloat16)

    for load in loads[6:]:
        load.wait()

    applied = jnp.concatenate(
        [
            visc_mat_ref[...].astype(jnp.float32).T.astype(jnp.bfloat16),
            pres_mat_ref[...].astype(jnp.float32).T.astype(jnp.bfloat16),
        ],
        axis=1,
    )

    for step, columns in enumerate(chunks):
        indices, sums = ready = prepared if step == 0 else prepare(step, columns)
        fill_owned(columns, HEAD if step == 0 else 0, owned_rows, ready)
        gathered[:, columns] = mul(sol_flip[...], table[pl.ds(0, owned_rows), columns])
        for slot in regions:
            first = owned_rows + slot * ghost_rows
            base = owned_rows + incoming[slot] * ghost_rows
            for start in range(0, ghost_rows, BLOCK):
                table[pl.ds(first + start, BLOCK), columns] = table_rows(
                    base + start, BLOCK, indices[1:], sums[1:]
                )
            table_flip[slot, columns, :] = table[pl.ds(first, ghost_rows), columns].T

    values = [gathered[:, columns] for columns in chunks]
    for group, first, count in (
        ((0, 1), 0, early),
        (range(2, len(pieces)), early, ghost_all - early),
    ):
        for number in group:

            @pl.when(has_source(number))
            def _():
                piece_copy(number).wait_recv()

        flipped = in_ghost[pl.ds(first, count), :].T
        values = [
            value + mul(flipped, table[pl.ds(owned_rows + first, count), columns])
            for value, columns in zip(values, chunks)
        ]
    pairs = []
    for value, columns in zip(values, chunks):
        element = value.astype(jnp.bfloat16)
        scaled = (element.astype(jnp.float32) * visc_ref[:, columns]).astype(jnp.bfloat16)
        pairs.append(jnp.concatenate([scaled, element], axis=0))
    for pair, columns in zip(pairs, chunks):
        elem_out[:, columns] = mul(applied, pair).astype(jnp.bfloat16)

    half = elem_rows // 2

    def scatter(region):
        return [
            mul(elem_out[:, rows], table_flip[region, rows, :])
            for rows in (pl.ds(0, half), pl.ds(half, half))
        ]

    back_order = [jnp.where(edge, 2, 1), jnp.where(edge, 1, 2)] + regions[3:] + [0]
    coming = scatter(back_order[0])
    for turn, slot in enumerate(back_order):
        front, back = coming
        if turn < region_count - 1:
            coming = scatter(back_order[turn + 1])
        out_part[part_rows(slot), :] = (front.T + back.T).astype(jnp.bfloat16)

        @pl.when(exists(me - offset_of(incoming_of(slot))))
        def _():
            part_copy(slot).start()

    local[...] = mul(elem_out[...], table[pl.ds(0, owned_rows), :], NT).T

    halves = [pl.ds(first, owned_rows // 2) for first in (0, owned_rows // 2)]
    totals = [local[rows, :] for rows in halves]
    for group in (regions[:2], regions[2:3], regions[3:]):
        for region in group:

            @pl.when(exists(me + offsets[region]))
            def _():
                part_arrival(region).wait_recv()

        totals = [
            total
            + sum(mul(mirror_table[region, rows, :], in_part[part_rows(region), :]) for region in group)
            for total, rows in zip(totals, halves)
        ]
    for total, rows in zip(totals, halves):
        result_ref[rows, :] = total

    for number in range(len(pieces)):

        @pl.when(has_target(number))
        def _():
            piece_copy(number).wait_send()

    for slot in regions:

        @pl.when(exists(me - offset_of(incoming_of(slot))))
        def _():
            part_copy(slot).wait_send()


def per_device(
    n_curve,
    n_seg,
    solution,
    viscosity,
    slot_index,
    slot_weight,
    mirror_rows,
    ghost_live,
    cell_count,
    viscous_block,
    pressure_block,
):
    owned_rows, width = solution.shape
    region_count, ghost_rows = mirror_rows.shape[1:]
    elem_rows = viscosity.shape[0]
    ghost_all = region_count * ghost_rows
    column_total = owned_rows + ghost_all
    vmem = pl.BlockSpec(memory_space=pltpu.VMEM)
    hbm = pl.BlockSpec(memory_space=pltpu.HBM)
    ghost_buffer = pltpu.VMEM((ghost_all, width), jnp.bfloat16)
    semaphores = pltpu.SemaphoreType.DMA((region_count,))
    piece_semaphores = pltpu.SemaphoreType.DMA((region_count + 1,))
    return pl.pallas_call(
        functools.partial(kernel, n_curve, n_seg, ghost_rows, region_count),
        out_shape=pltpu.VMEM((owned_rows, width), jnp.float32),
        in_specs=[hbm] * 9,
        out_specs=vmem,
        scratch_shapes=[
            pltpu.VMEM(solution.shape, solution.dtype),
            pltpu.VMEM((1, elem_rows), viscosity.dtype),
            pltpu.VMEM(slot_index.shape[::-1], slot_index.dtype),
            pltpu.VMEM(slot_weight.shape[::-1], slot_weight.dtype),
            pltpu.VMEM(mirror_rows.shape[1:], mirror_rows.dtype),
            pltpu.SMEM(ghost_live.shape, ghost_live.dtype),
            pltpu.VMEM(viscous_block.shape, viscous_block.dtype),
            pltpu.VMEM(pressure_block.shape, pressure_block.dtype),
            pltpu.SMEM(cell_count.shape, cell_count.dtype),
            pltpu.SemaphoreType.DMA((9,)),
            pltpu.VMEM((width, owned_rows), jnp.bfloat16),
            pltpu.VMEM((owned_rows, width), jnp.float32),
            pltpu.VMEM((column_total, elem_rows), jnp.bfloat16),
            pltpu.VMEM((region_count, elem_rows, ghost_rows), jnp.bfloat16),
            pltpu.VMEM((width, elem_rows), jnp.float32),
            pltpu.VMEM((width, elem_rows), jnp.bfloat16),
            pltpu.VMEM((region_count, owned_rows, ghost_rows), jnp.bfloat16),
            ghost_buffer,
            ghost_buffer,
            ghost_buffer,
            ghost_buffer,
            piece_semaphores,
            piece_semaphores,
            semaphores,
            semaphores,
        ],
        compiler_params=pltpu.CompilerParams(
            collective_id=0, has_side_effects=True, vmem_limit_bytes=60 * 1024 * 1024
        ),
        name="stokes_operator",
    )(
        solution,
        viscosity.reshape(1, elem_rows),
        slot_index.T,
        slot_weight.T,
        mirror_rows[0],
        ghost_live,
        cell_count,
        viscous_block,
        pressure_block,
    )


def solution(mesh):
    return jax.shard_map(
        functools.partial(per_device, mesh.shape["curve"], mesh.shape["seg"]),
        mesh=mesh,
        in_specs=(
            P(("curve", "seg"), None),
            P(("curve", "seg")),
            P(("curve", "seg"), None),
            P(("curve", "seg"), None),
            P(("curve", "seg"), None, None),
            P(("curve", "seg"), None),
            P(("curve", "seg")),
            P(),
            P(),
        ),
        out_specs=P(("curve", "seg"), None),
        check_vma=False,
    )
```

```python
import functools

import jax
import jax.numpy as jnp
from jax import lax
from jax.experimental import pallas as pl
from jax.experimental.pallas import tpu as pltpu
from jax.sharding import PartitionSpec as P

CHUNK = 512
GROUP = 16
BLOCK = 64
TILE = 256
HEAD = 128
NN = (((1,), (0,)), ((), ()))
NT = (((1,), (1,)), ((), ()))
TN = (((0,), (0,)), ((), ()))


def shift_list(region_count):
    return [(region // 2 + 1) * (1 if region % 2 == 0 else -1) for region in range(region_count)]


def mul(left, right, dims=NN):
    return lax.dot_general(left, right, dims, preferred_element_type=jnp.float32)


def kernel(
    n_curve,
    n_seg,
    ghost_rows,
    region_count,
    sol_in,
    visc_in,
    index_in,
    code_in,
    mirror_in,
    live_in,
    count_in,
    visc_mat_in,
    pres_mat_in,
    result_ref,
    sol_ref,
    visc_ref,
    index_ref,
    code_ref,
    mirror_ref,
    live_ref,
    visc_mat_ref,
    pres_mat_ref,
    count_ref,
    load_sem,
    sol_flip,
    local,
    table,
    table_flip,
    gathered,
    elem_out,
    mirror_table,
    out_ghost,
    in_ghost,
    out_part,
    in_part,
    send_sem,
    recv_sem,
    send_back_sem,
    recv_back_sem,
):
    pairs = (
        (mirror_in, mirror_ref),
        (live_in, live_ref),
        (sol_in, sol_ref),
        (count_in, count_ref),
        (index_in, index_ref),
        (code_in, code_ref),
        (visc_mat_in, visc_mat_ref),
        (pres_mat_in, pres_mat_ref),
        (visc_in, visc_ref),
    )
    devices_all = n_curve * n_seg
    owned_rows, width = sol_ref.shape
    slot_total, elem_rows = index_ref.shape
    chunk = min(CHUNK, elem_rows)
    ghost_all = ghost_rows * region_count
    offsets = shift_list(region_count)
    me = lax.axis_index("curve") * n_seg + lax.axis_index("seg")

    def exists(other):
        return jnp.logical_and(other >= 0, other < devices_all)

    def place(other):
        safe = jnp.clip(other, 0, devices_all - 1)
        return (safe // n_seg, safe % n_seg)

    barrier = pltpu.get_barrier_semaphore()
    for offset in offsets[::-1]:

        @pl.when(exists(me + offset))
        def _():
            pl.semaphore_signal(
                barrier,
                inc=1,
                device_id=place(me + offset),
                device_id_type=pl.DeviceIdType.MESH,
            )

    loads = [
        pltpu.make_async_copy(source, target, load_sem.at[position])
        for position, (source, target) in enumerate(pairs)
    ]
    for load in loads:
        load.start()

    for load in loads[:6]:
        load.wait()

    def table_rows(start, total, indices, weights):
        shape = (total // GROUP, GROUP, chunk)
        position = (
            lax.broadcasted_iota(jnp.int32, shape, 0) * GROUP
            + lax.broadcasted_iota(jnp.int32, shape, 1)
            + start
        ).astype(jnp.int16)
        value = jnp.zeros(shape, jnp.bfloat16)
        for index, weight in zip(indices, weights):
            hit = position == jnp.broadcast_to(index[None], shape)
            value = jnp.where(hit, jnp.broadcast_to(weight[None], shape), value)
        return value.reshape(total, chunk)

    chunks = [pl.ds(first, chunk) for first in range(0, elem_rows, chunk)]

    def prepare(step, columns):
        element = lax.broadcasted_iota(jnp.int32, (1, chunk), 1) + step * chunk
        alive = element < count_ref[0]
        indices, weights = [], []
        for slot in range(slot_total):
            index = index_ref[slot : slot + 1, columns]
            code = code_ref[slot : slot + 1, columns].astype(jnp.float32) * 0.125
            weight = jnp.where(alive, code, 0.0)
            indices.append(jnp.broadcast_to(index, (GROUP, chunk)).astype(jnp.int16))
            weights.append(jnp.broadcast_to(weight, (GROUP, chunk)).astype(jnp.bfloat16))
        sums = []
        for slot in range(slot_total):
            value = weights[slot]
            for other in range(slot):
                same = indices[other] == indices[slot]
                value = value + jnp.where(same, weights[other], jnp.zeros_like(value))
            sums.append(value)
        return indices, sums

    def fill_owned(columns, first, last, ready):
        for start in range(first, last, BLOCK):
            table[pl.ds(start, BLOCK), columns] = table_rows(start, BLOCK, *ready)

    sol_flip[...] = sol_ref[...].T

    lanes = lax.broadcasted_iota(jnp.int32, (1, ghost_rows), 1)
    shape = (owned_rows // GROUP, GROUP, ghost_rows)
    position = (
        lax.broadcasted_iota(jnp.int32, shape, 0) * GROUP
        + lax.broadcasted_iota(jnp.int32, shape, 1)
    ).astype(jnp.int16)
    for region in range(region_count):
        listed = jnp.where(
            lanes < live_ref[0, region], mirror_ref[region : region + 1, :], -1
        )
        listed = jnp.broadcast_to(listed, (GROUP, ghost_rows)).astype(jnp.int16)
        hit = position == jnp.broadcast_to(listed[None], shape)
        chosen = jnp.where(hit, jnp.ones(shape, jnp.bfloat16), jnp.zeros(shape, jnp.bfloat16))
        mirror_table[region] = chosen.reshape(owned_rows, ghost_rows)
        out_ghost[pl.ds(region * ghost_rows, ghost_rows), :] = mul(
            sol_flip[...], mirror_table[region]
        ).T.astype(jnp.bfloat16)

    prepared = prepare(0, chunks[0])
    fill_owned(chunks[0], 0, HEAD, prepared)

    def offset_of(region):
        return (region // 2 + 1) * (1 - 2 * (region % 2))

    def part_rows(region):
        return pl.ds(pl.multiple_of(region * ghost_rows, GROUP), ghost_rows)

    regions = list(range(region_count))
    edge = me < n_seg
    odd = me % 2
    incoming = [1 - odd, odd] + regions[2:]
    outgoing = [odd, 1 - odd] + regions[2:]
    lead = -ghost_rows % TILE
    early = ghost_rows + lead
    pieces = [(0, 0, ghost_rows), (1, 0, lead), (1, lead, ghost_rows - lead)]
    pieces += [(slot, 0, ghost_rows) for slot in regions[2:]]

    def piece_copy(number):
        slot, first, count = pieces[number]
        source = pl.multiple_of(outgoing[slot] * ghost_rows + first, GROUP)
        return pltpu.make_async_remote_copy(
            src_ref=out_ghost.at[pl.ds(source, count)],
            dst_ref=in_ghost.at[pl.ds(slot * ghost_rows + first, count)],
            send_sem=send_sem.at[number],
            recv_sem=recv_sem.at[number],
            device_id=place(me + offset_of(outgoing[slot])),
            device_id_type=pl.DeviceIdType.MESH,
        )

    def has_target(number):
        return exists(me + offset_of(outgoing[pieces[number][0]]))

    def has_source(number):
        return exists(me - offset_of(incoming[pieces[number][0]]))

    def incoming_of(slot):
        return jnp.where(slot < 2, (1 - slot) * (1 - odd) + slot * odd, slot)

    def part_copy(slot):
        region = incoming_of(slot)
        return pltpu.make_async_remote_copy(
            src_ref=out_part.at[part_rows(slot)],
            dst_ref=in_part.at[part_rows(region)],
            send_sem=send_back_sem.at[slot],
            recv_sem=recv_back_sem.at[region],
            device_id=place(me - offset_of(region)),
            device_id_type=pl.DeviceIdType.MESH,
        )

    def part_arrival(region):
        return pltpu.make_async_remote_copy(
            src_ref=out_part.at[part_rows(region)],
            dst_ref=in_part.at[part_rows(region)],
            send_sem=send_back_sem.at[region],
            recv_sem=recv_back_sem.at[region],
            device_id=place(me + offsets[region]),
            device_id_type=pl.DeviceIdType.MESH,
        )

    peers = sum(jnp.where(exists(me + offset), 1, 0) for offset in offsets)
    pl.semaphore_wait(barrier, peers)

    for number in (1, 0, 2, *range(len(pieces) - 1, 2, -1)):

        @pl.when(has_target(number))
        def _():
            piece_copy(number).start()

    for number, (slot, first, count) in enumerate(pieces):

        @pl.when(jnp.logical_not(has_source(number)))
        def _():
            in_ghost[pl.ds(slot * ghost_rows + first, count), :] = jnp.zeros(
                (count, width), jnp.bfloat16
            )

    for region, offset in enumerate(offsets):

        @pl.when(jnp.logical_not(exists(me + offset)))
        def _():
            in_part[part_rows(region), :] = jnp.zeros((ghost_rows, width), jnp.bfloat16)

    for load in loads[6:]:
        load.wait()

    applied = jnp.concatenate(
        [
            visc_mat_ref[...].astype(jnp.float32).T.astype(jnp.bfloat16),
            pres_mat_ref[...].astype(jnp.float32).T.astype(jnp.bfloat16),
        ],
        axis=1,
    )

    for step, columns in enumerate(chunks):
        indices, sums = ready = prepared if step == 0 else prepare(step, columns)
        fill_owned(columns, HEAD if step == 0 else 0, owned_rows, ready)
        gathered[:, columns] = mul(sol_flip[...], table[pl.ds(0, owned_rows), columns])
        for slot in regions:
            first = owned_rows + slot * ghost_rows
            base = owned_rows + incoming[slot] * ghost_rows
            for start in range(0, ghost_rows, BLOCK):
                table[pl.ds(first + start, BLOCK), columns] = table_rows(
                    base + start, BLOCK, indices[1:], sums[1:]
                )
            table_flip[slot, columns, :] = table[pl.ds(first, ghost_rows), columns].T

    values = [gathered[:, columns] for columns in chunks]
    for group, first, count in (
        ((0, 1), 0, early),
        (range(2, len(pieces)), early, ghost_all - early),
    ):
        for number in group:

            @pl.when(has_source(number))
            def _():
                piece_copy(number).wait_recv()

        flipped = in_ghost[pl.ds(first, count), :].T
        values = [
            value + mul(flipped, table[pl.ds(owned_rows + first, count), columns])
            for value, columns in zip(values, chunks)
        ]
    pairs = []
    for value, columns in zip(values, chunks):
        element = value.astype(jnp.bfloat16)
        scaled = (element.astype(jnp.float32) * visc_ref[:, columns]).astype(jnp.bfloat16)
        pairs.append(jnp.concatenate([scaled, element], axis=0))
    for pair, columns in zip(pairs, chunks):
        elem_out[:, columns] = mul(applied, pair).astype(jnp.bfloat16)

    half = elem_rows // 2

    def scatter(region):
        return [
            mul(elem_out[:, rows], table_flip[region, rows, :])
            for rows in (pl.ds(0, half), pl.ds(half, half))
        ]

    back_order = [jnp.where(edge, 2, 1), jnp.where(edge, 1, 2)] + regions[3:] + [0]
    coming = scatter(back_order[0])
    for turn, slot in enumerate(back_order):
        front, back = coming
        if turn < region_count - 1:
            coming = scatter(back_order[turn + 1])
        front, back = (half_sum.astype(jnp.bfloat16).T for half_sum in (front, back))
        out_part[part_rows(slot), :] = front + back

        @pl.when(exists(me - offset_of(incoming_of(slot))))
        def _():
            part_copy(slot).start()

    local[...] = mul(elem_out[...], table[pl.ds(0, owned_rows), :], NT).T

    halves = [pl.ds(first, owned_rows // 2) for first in (0, owned_rows // 2)]
    totals = [local[rows, :] for rows in halves]
    for group in (regions[:2], regions[2:3], regions[3:]):
        for region in group:

            @pl.when(exists(me + offsets[region]))
            def _():
                part_arrival(region).wait_recv()

        totals = [
            total
            + sum(mul(mirror_table[region, rows, :], in_part[part_rows(region), :]) for region in group)
            for total, rows in zip(totals, halves)
        ]
    for total, rows in zip(totals, halves):
        result_ref[rows, :] = total

    for number in range(len(pieces)):

        @pl.when(has_target(number))
        def _():
            piece_copy(number).wait_send()

    for slot in regions:

        @pl.when(exists(me - offset_of(incoming_of(slot))))
        def _():
            part_copy(slot).wait_send()


def per_device(
    n_curve,
    n_seg,
    solution,
    viscosity,
    slot_index,
    slot_weight,
    mirror_rows,
    ghost_live,
    cell_count,
    viscous_block,
    pressure_block,
):
    owned_rows, width = solution.shape
    region_count, ghost_rows = mirror_rows.shape[1:]
    elem_rows = viscosity.shape[0]
    ghost_all = region_count * ghost_rows
    column_total = owned_rows + ghost_all
    vmem = pl.BlockSpec(memory_space=pltpu.VMEM)
    hbm = pl.BlockSpec(memory_space=pltpu.HBM)
    ghost_buffer = pltpu.VMEM((ghost_all, width), jnp.bfloat16)
    semaphores = pltpu.SemaphoreType.DMA((region_count,))
    piece_semaphores = pltpu.SemaphoreType.DMA((region_count + 1,))
    return pl.pallas_call(
        functools.partial(kernel, n_curve, n_seg, ghost_rows, region_count),
        out_shape=pltpu.VMEM((owned_rows, width), jnp.float32),
        in_specs=[hbm] * 9,
        out_specs=vmem,
        scratch_shapes=[
            pltpu.VMEM(solution.shape, solution.dtype),
            pltpu.VMEM((1, elem_rows), viscosity.dtype),
            pltpu.VMEM(slot_index.shape[::-1], slot_index.dtype),
            pltpu.VMEM(slot_weight.shape[::-1], slot_weight.dtype),
            pltpu.VMEM(mirror_rows.shape[1:], mirror_rows.dtype),
            pltpu.SMEM(ghost_live.shape, ghost_live.dtype),
            pltpu.VMEM(viscous_block.shape, viscous_block.dtype),
            pltpu.VMEM(pressure_block.shape, pressure_block.dtype),
            pltpu.SMEM(cell_count.shape, cell_count.dtype),
            pltpu.SemaphoreType.DMA((9,)),
            pltpu.VMEM((width, owned_rows), jnp.bfloat16),
            pltpu.VMEM((owned_rows, width), jnp.float32),
            pltpu.VMEM((column_total, elem_rows), jnp.bfloat16),
            pltpu.VMEM((region_count, elem_rows, ghost_rows), jnp.bfloat16),
            pltpu.VMEM((width, elem_rows), jnp.float32),
            pltpu.VMEM((width, elem_rows), jnp.bfloat16),
            pltpu.VMEM((region_count, owned_rows, ghost_rows), jnp.bfloat16),
            ghost_buffer,
            ghost_buffer,
            ghost_buffer,
            ghost_buffer,
            piece_semaphores,
            piece_semaphores,
            semaphores,
            semaphores,
        ],
        compiler_params=pltpu.CompilerParams(
            collective_id=0,
            has_side_effects=True,
            vmem_limit_bytes=60 * 1024 * 1024,
        ),
        name="stokes_operator",
    )(
        solution,
        viscosity.reshape(1, elem_rows),
        slot_index.T,
        slot_weight.T,
        mirror_rows[0],
        ghost_live,
        cell_count,
        viscous_block,
        pressure_block,
    )


def solution(mesh):
    return jax.shard_map(
        functools.partial(per_device, mesh.shape["curve"], mesh.shape["seg"]),
        mesh=mesh,
        in_specs=(
            P(("curve", "seg"), None),
            P(("curve", "seg")),
            P(("curve", "seg"), None),
            P(("curve", "seg"), None),
            P(("curve", "seg"), None, None),
            P(("curve", "seg"), None),
            P(("curve", "seg")),
            P(),
            P(),
        ),
        out_specs=P(("curve", "seg"), None),
        check_vma=False,
    )
```

```python
import functools

import jax
import jax.numpy as jnp
from jax import lax
from jax.experimental import pallas as pl
from jax.experimental.pallas import tpu as pltpu
from jax.sharding import PartitionSpec as P

CHUNK = 1024
GROUP = 16
BLOCK = 64
TILE = 256
HEAD = 128
NN = (((1,), (0,)), ((), ()))
NT = (((1,), (1,)), ((), ()))
TN = (((0,), (0,)), ((), ()))


def shift_list(region_count):
    return [(region // 2 + 1) * (1 if region % 2 == 0 else -1) for region in range(region_count)]


def mul(left, right, dims=NN):
    return lax.dot_general(left, right, dims, preferred_element_type=jnp.float32)


def kernel(
    n_curve,
    n_seg,
    ghost_rows,
    region_count,
    sol_in,
    visc_in,
    index_in,
    code_in,
    mirror_in,
    live_in,
    count_in,
    visc_mat_in,
    pres_mat_in,
    result_ref,
    sol_ref,
    visc_ref,
    index_ref,
    code_ref,
    mirror_ref,
    live_ref,
    visc_mat_ref,
    pres_mat_ref,
    count_ref,
    load_sem,
    sol_flip,
    local,
    table,
    table_flip,
    gathered,
    elem_out,
    mirror_table,
    out_ghost,
    in_ghost,
    out_part,
    in_part,
    send_sem,
    recv_sem,
    send_back_sem,
    recv_back_sem,
):
    pairs = (
        (mirror_in, mirror_ref),
        (live_in, live_ref),
        (sol_in, sol_ref),
        (count_in, count_ref),
        (index_in, index_ref),
        (code_in, code_ref),
        (visc_mat_in, visc_mat_ref),
        (pres_mat_in, pres_mat_ref),
        (visc_in, visc_ref),
    )
    devices_all = n_curve * n_seg
    owned_rows, width = sol_ref.shape
    slot_total, elem_rows = index_ref.shape
    chunk = min(CHUNK, elem_rows)
    ghost_all = ghost_rows * region_count
    offsets = shift_list(region_count)
    me = lax.axis_index("curve") * n_seg + lax.axis_index("seg")

    def exists(other):
        return jnp.logical_and(other >= 0, other < devices_all)

    def place(other):
        safe = jnp.clip(other, 0, devices_all - 1)
        return (safe // n_seg, safe % n_seg)

    barrier = pltpu.get_barrier_semaphore()
    for offset in offsets[::-1]:

        @pl.when(exists(me + offset))
        def _():
            pl.semaphore_signal(
                barrier,
                inc=1,
                device_id=place(me + offset),
                device_id_type=pl.DeviceIdType.MESH,
            )

    loads = [
        pltpu.make_async_copy(source, target, load_sem.at[position])
        for position, (source, target) in enumerate(pairs)
    ]
    for load in loads:
        load.start()

    for load in loads[:6]:
        load.wait()

    def table_rows(start, total, indices, weights):
        shape = (total // GROUP, GROUP, chunk)
        position = (
            lax.broadcasted_iota(jnp.int32, shape, 0) * GROUP
            + lax.broadcasted_iota(jnp.int32, shape, 1)
            + start
        ).astype(jnp.int16)
        value = jnp.zeros(shape, jnp.bfloat16)
        for index, weight in zip(indices, weights):
            hit = position == jnp.broadcast_to(index[None], shape)
            value = jnp.where(hit, jnp.broadcast_to(weight[None], shape), value)
        return value.reshape(total, chunk)

    chunks = [pl.ds(first, chunk) for first in range(0, elem_rows, chunk)]

    def prepare(step, columns):
        element = lax.broadcasted_iota(jnp.int32, (1, chunk), 1) + step * chunk
        alive = element < count_ref[0]
        indices, weights = [], []
        for slot in range(slot_total):
            index = index_ref[slot : slot + 1, columns]
            code = code_ref[slot : slot + 1, columns].astype(jnp.float32) * 0.125
            weight = jnp.where(alive, code, 0.0)
            indices.append(jnp.broadcast_to(index, (GROUP, chunk)).astype(jnp.int16))
            weights.append(jnp.broadcast_to(weight, (GROUP, chunk)).astype(jnp.bfloat16))
        sums = []
        for slot in range(slot_total):
            value = weights[slot]
            for other in range(slot):
                same = indices[other] == indices[slot]
                value = value + jnp.where(same, weights[other], jnp.zeros_like(value))
            sums.append(value)
        return indices, sums

    def fill_owned(columns, first, last, ready):
        for start in range(first, last, BLOCK):
            table[pl.ds(start, BLOCK), columns] = table_rows(start, BLOCK, *ready)

    sol_flip[...] = sol_ref[...].T

    lanes = lax.broadcasted_iota(jnp.int32, (1, ghost_rows), 1)
    shape = (owned_rows // GROUP, GROUP, ghost_rows)
    position = (
        lax.broadcasted_iota(jnp.int32, shape, 0) * GROUP
        + lax.broadcasted_iota(jnp.int32, shape, 1)
    ).astype(jnp.int16)
    for region in range(region_count):
        listed = jnp.where(
            lanes < live_ref[0, region], mirror_ref[region : region + 1, :], -1
        )
        listed = jnp.broadcast_to(listed, (GROUP, ghost_rows)).astype(jnp.int16)
        hit = position == jnp.broadcast_to(listed[None], shape)
        chosen = jnp.where(hit, jnp.ones(shape, jnp.bfloat16), jnp.zeros(shape, jnp.bfloat16))
        mirror_table[region] = chosen.reshape(owned_rows, ghost_rows)
        out_ghost[pl.ds(region * ghost_rows, ghost_rows), :] = mul(
            sol_flip[...], mirror_table[region]
        ).T.astype(jnp.bfloat16)

    prepared = prepare(0, chunks[0])
    fill_owned(chunks[0], 0, HEAD, prepared)

    def offset_of(region):
        return (region // 2 + 1) * (1 - 2 * (region % 2))

    def part_rows(region):
        return pl.ds(pl.multiple_of(region * ghost_rows, GROUP), ghost_rows)

    regions = list(range(region_count))
    edge = me < n_seg
    odd = me % 2
    incoming = [1 - odd, odd] + regions[2:]
    outgoing = [odd, 1 - odd] + regions[2:]
    lead = -ghost_rows % TILE
    early = ghost_rows + lead
    pieces = [(0, 0, ghost_rows), (1, 0, lead), (1, lead, ghost_rows - lead)]
    pieces += [(slot, 0, ghost_rows) for slot in regions[2:]]

    def piece_copy(number):
        slot, first, count = pieces[number]
        source = pl.multiple_of(outgoing[slot] * ghost_rows + first, GROUP)
        return pltpu.make_async_remote_copy(
            src_ref=out_ghost.at[pl.ds(source, count)],
            dst_ref=in_ghost.at[pl.ds(slot * ghost_rows + first, count)],
            send_sem=send_sem.at[number],
            recv_sem=recv_sem.at[number],
            device_id=place(me + offset_of(outgoing[slot])),
            device_id_type=pl.DeviceIdType.MESH,
        )

    def has_target(number):
        return exists(me + offset_of(outgoing[pieces[number][0]]))

    def has_source(number):
        return exists(me - offset_of(incoming[pieces[number][0]]))

    def incoming_of(slot):
        return jnp.where(slot < 2, (1 - slot) * (1 - odd) + slot * odd, slot)

    def part_copy(slot):
        region = incoming_of(slot)
        return pltpu.make_async_remote_copy(
            src_ref=out_part.at[part_rows(slot)],
            dst_ref=in_part.at[part_rows(region)],
            send_sem=send_back_sem.at[slot],
            recv_sem=recv_back_sem.at[region],
            device_id=place(me - offset_of(region)),
            device_id_type=pl.DeviceIdType.MESH,
        )

    def part_arrival(region):
        return pltpu.make_async_remote_copy(
            src_ref=out_part.at[part_rows(region)],
            dst_ref=in_part.at[part_rows(region)],
            send_sem=send_back_sem.at[region],
            recv_sem=recv_back_sem.at[region],
            device_id=place(me + offsets[region]),
            device_id_type=pl.DeviceIdType.MESH,
        )

    peers = sum(jnp.where(exists(me + offset), 1, 0) for offset in offsets)
    pl.semaphore_wait(barrier, peers)

    for number in (1, 2, *range(len(pieces) - 1, 2, -1), 0):

        @pl.when(has_target(number))
        def _():
            piece_copy(number).start()

    for number, (slot, first, count) in enumerate(pieces):

        @pl.when(jnp.logical_not(has_source(number)))
        def _():
            in_ghost[pl.ds(slot * ghost_rows + first, count), :] = jnp.zeros(
                (count, width), jnp.bfloat16
            )

    for region, offset in enumerate(offsets):

        @pl.when(jnp.logical_not(exists(me + offset)))
        def _():
            in_part[part_rows(region), :] = jnp.zeros((ghost_rows, width), jnp.bfloat16)

    for load in loads[6:]:
        load.wait()

    applied = jnp.concatenate(
        [
            visc_mat_ref[...].astype(jnp.float32).T.astype(jnp.bfloat16),
            pres_mat_ref[...].astype(jnp.float32).T.astype(jnp.bfloat16),
        ],
        axis=1,
    )

    for step, columns in enumerate(chunks):
        indices, sums = ready = prepared if step == 0 else prepare(step, columns)
        fill_owned(columns, HEAD if step == 0 else 0, owned_rows, ready)
        gathered[:, columns] = mul(sol_flip[...], table[pl.ds(0, owned_rows), columns])
        for slot in regions:
            first = owned_rows + slot * ghost_rows
            base = owned_rows + incoming[slot] * ghost_rows
            for start in range(0, ghost_rows, BLOCK):
                table[pl.ds(first + start, BLOCK), columns] = table_rows(
                    base + start, BLOCK, indices[1:], sums[1:]
                )
            table_flip[slot, columns, :] = table[pl.ds(first, ghost_rows), columns].T

    values = [gathered[:, columns] for columns in chunks]
    for group, first, count in (
        ((0, 1), 0, early),
        (range(2, len(pieces)), early, ghost_all - early),
    ):
        for number in group:

            @pl.when(has_source(number))
            def _():
                piece_copy(number).wait_recv()

        flipped = in_ghost[pl.ds(first, count), :].T
        values = [
            value + mul(flipped, table[pl.ds(owned_rows + first, count), columns])
            for value, columns in zip(values, chunks)
        ]
    pairs = []
    for value, columns in zip(values, chunks):
        element = value.astype(jnp.bfloat16)
        scaled = (element.astype(jnp.float32) * visc_ref[:, columns]).astype(jnp.bfloat16)
        pairs.append(jnp.concatenate([scaled, element], axis=0))
    for pair, columns in zip(pairs, chunks):
        elem_out[:, columns] = mul(applied, pair).astype(jnp.bfloat16)

    half = elem_rows // 2

    def scatter(region):
        return [
            mul(elem_out[:, rows], table_flip[region, rows, :])
            for rows in (pl.ds(0, half), pl.ds(half, half))
        ]

    back_order = [jnp.where(edge, 2, 1), jnp.where(edge, 1, 2)] + regions[3:] + [0]
    coming = scatter(back_order[0])
    for turn, slot in enumerate(back_order):
        front, back = coming
        if turn < region_count - 1:
            coming = scatter(back_order[turn + 1])
        out_part[part_rows(slot), :] = (front.T + back.T).astype(jnp.bfloat16)

        @pl.when(exists(me - offset_of(incoming_of(slot))))
        def _():
            part_copy(slot).start()

    local[...] = mul(elem_out[...], table[pl.ds(0, owned_rows), :], NT).T

    halves = [pl.ds(first, owned_rows // 2) for first in (0, owned_rows // 2)]
    totals = [local[rows, :] for rows in halves]
    for group in (regions[:2], regions[2:3], regions[3:]):
        for region in group:

            @pl.when(exists(me + offsets[region]))
            def _():
                part_arrival(region).wait_recv()

        totals = [
            total
            + sum(mul(mirror_table[region, rows, :], in_part[part_rows(region), :]) for region in group)
            for total, rows in zip(totals, halves)
        ]
    for total, rows in zip(totals, halves):
        result_ref[rows, :] = total

    for number in range(len(pieces)):

        @pl.when(has_target(number))
        def _():
            piece_copy(number).wait_send()

    for slot in regions:

        @pl.when(exists(me - offset_of(incoming_of(slot))))
        def _():
            part_copy(slot).wait_send()


def per_device(
    n_curve,
    n_seg,
    solution,
    viscosity,
    slot_index,
    slot_weight,
    mirror_rows,
    ghost_live,
    cell_count,
    viscous_block,
    pressure_block,
):
    owned_rows, width = solution.shape
    region_count, ghost_rows = mirror_rows.shape[1:]
    elem_rows = viscosity.shape[0]
    ghost_all = region_count * ghost_rows
    column_total = owned_rows + ghost_all
    vmem = pl.BlockSpec(memory_space=pltpu.VMEM)
    hbm = pl.BlockSpec(memory_space=pltpu.HBM)
    ghost_buffer = pltpu.VMEM((ghost_all, width), jnp.bfloat16)
    semaphores = pltpu.SemaphoreType.DMA((region_count,))
    piece_semaphores = pltpu.SemaphoreType.DMA((region_count + 1,))
    return pl.pallas_call(
        functools.partial(kernel, n_curve, n_seg, ghost_rows, region_count),
        out_shape=pltpu.VMEM((owned_rows, width), jnp.float32),
        in_specs=[hbm] * 9,
        out_specs=vmem,
        scratch_shapes=[
            pltpu.VMEM(solution.shape, solution.dtype),
            pltpu.VMEM((1, elem_rows), viscosity.dtype),
            pltpu.VMEM(slot_index.shape[::-1], slot_index.dtype),
            pltpu.VMEM(slot_weight.shape[::-1], slot_weight.dtype),
            pltpu.VMEM(mirror_rows.shape[1:], mirror_rows.dtype),
            pltpu.SMEM(ghost_live.shape, ghost_live.dtype),
            pltpu.VMEM(viscous_block.shape, viscous_block.dtype),
            pltpu.VMEM(pressure_block.shape, pressure_block.dtype),
            pltpu.SMEM(cell_count.shape, cell_count.dtype),
            pltpu.SemaphoreType.DMA((9,)),
            pltpu.VMEM((width, owned_rows), jnp.bfloat16),
            pltpu.VMEM((owned_rows, width), jnp.float32),
            pltpu.VMEM((column_total, elem_rows), jnp.bfloat16),
            pltpu.VMEM((region_count, elem_rows, ghost_rows), jnp.bfloat16),
            pltpu.VMEM((width, elem_rows), jnp.float32),
            pltpu.VMEM((width, elem_rows), jnp.bfloat16),
            pltpu.VMEM((region_count, owned_rows, ghost_rows), jnp.bfloat16),
            ghost_buffer,
            ghost_buffer,
            ghost_buffer,
            ghost_buffer,
            piece_semaphores,
            piece_semaphores,
            semaphores,
            semaphores,
        ],
        compiler_params=pltpu.CompilerParams(
            collective_id=0, has_side_effects=True, vmem_limit_bytes=60 * 1024 * 1024
        ),
        name="stokes_operator",
    )(
        solution,
        viscosity.reshape(1, elem_rows),
        slot_index.T,
        slot_weight.T,
        mirror_rows[0],
        ghost_live,
        cell_count,
        viscous_block,
        pressure_block,
    )


def solution(mesh):
    return jax.shard_map(
        functools.partial(per_device, mesh.shape["curve"], mesh.shape["seg"]),
        mesh=mesh,
        in_specs=(
            P(("curve", "seg"), None),
            P(("curve", "seg")),
            P(("curve", "seg"), None),
            P(("curve", "seg"), None),
            P(("curve", "seg"), None, None),
            P(("curve", "seg"), None),
            P(("curve", "seg")),
            P(),
            P(),
        ),
        out_specs=P(("curve", "seg"), None),
        check_vma=False,
    )
```
